512 devices in a mesh: sp: 64 (over z_lo, x, core), dp: 8 (over y, z_hi).
Axes of the slice: x: 4, y: 4, z: 16 (z_hi: 2, z_lo: 8; z = z_hi * 8 + z_lo), core: 2. Of those that a mesh axis runs over, the one named last changes fastest.
Arguments:
- queries: bfloat16 [24576, 24, 128], P(('dp', 'sp')), parts along dimension 0, may hold values from -12 to 12
- keys: bfloat16 [24576, 24, 128], P(('dp', 'sp')), parts along dimension 0, may hold values from -6 to 6
- values: bfloat16 [24576, 24, 128], P(('dp', 'sp')), parts along dimension 0, may hold values from -6 to 6
Outputs:
- attended: bfloat16 [24576, 3072], P(('dp', 'sp')), parts along dimension 0
The draws below stay inside these ranges and needn't reach their ends.
There are 8 independent parts, one for each index of `dp`. The reference program is written for one: setup_inputs(seed, part) draws one part's arguments, and reference() takes and returns one part's arrays. A program takes and returns all parts, laid end to end along the dimension named above; each array names one. Nothing has to cross between parts.
All inputs are finite; a program needn't handle non-finite values.
Results may differ from the reference program's by a relative error of at most 0.0049.
Values may be sent and summed in bfloat16 or wider, within the bound.
A program may use at most 64 MiB of HBM per device.

```python
import jax
import jax.numpy as jnp
from jax import lax

HEADS = 24
HEAD_DIM = 128
SEQ = 3072


def draw_queries(key, part):
    own_key = jax.random.fold_in(key, 1)
    result = 2.5 * jax.random.truncated_normal(own_key, -4.8, 4.8, (SEQ, HEADS, HEAD_DIM), jnp.float32)
    return result.astype(jnp.bfloat16)


def draw_keys(key, part):
    own_key = jax.random.fold_in(key, 2)
    result = jax.random.truncated_normal(own_key, -6.0, 6.0, (SEQ, HEADS, HEAD_DIM), jnp.float32)
    return result.astype(jnp.bfloat16)


def levels(rng, extent, pieces, least, largest):
    level, own = 1.0, jax.random.fold_in(rng, 6)
    for position, shards_of in pieces:
        steps = jnp.exp(jax.random.uniform(jax.random.fold_in(own, position), (shards_of,), jnp.float32, least / len(pieces), largest / len(pieces)))
        level = level * jnp.repeat(steps, extent[position] // shards_of).reshape([-1 if axis == position else 1 for axis in range(len(extent))])
    return level


def gaussian(stream_key, shape, scale, bound, pieces=(), dtype=jnp.bfloat16):
    drawn = jax.random.normal(stream_key, shape, jnp.float32) * scale
    if len(pieces) > 0:
        drawn = levels(stream_key, shape, pieces, -0.22, 0.18) * drawn
    return jnp.clip(drawn, min=-bound, max=bound).astype(dtype)


def setup_inputs(seed: int = 0, part: int = 0) -> dict:
    splits = jax.random.split(jax.random.key(seed), 4)
    part_keys = jax.random.split(jax.random.fold_in(splits[3], part), 4)
    return {
        "queries": draw_queries(jax.random.fold_in(jax.random.fold_in(splits[3], part), 71), part),
        "keys": draw_keys(jax.random.fold_in(jax.random.fold_in(splits[3], part), 71), part),
        "values": gaussian(part_keys[2], (SEQ, HEADS, HEAD_DIM), 1.0, 6.0, ((0, 64),)),
    }


def attend(triple):
    head_q, head_k, head_v = triple
    scale = 1.0 / (head_q.shape[-1] ** 0.5)
    scores = jnp.dot(head_q, head_k.T, preferred_element_type=jnp.float32) * scale
    weights = jax.nn.softmax(scores, axis=-1).astype(jnp.bfloat16)
    return jnp.dot(weights, head_v, preferred_element_type=jnp.float32)


def reference(queries, keys, values):
    seq_len, heads, width = queries.shape
    result = lax.map(attend, (queries.transpose(1, 0, 2), keys.transpose(1, 0, 2), values.transpose(1, 0, 2)))
    return result.transpose(1, 0, 2).reshape(seq_len, heads * width).astype(jnp.bfloat16)
```

```python
import functools
import math

import jax
import jax.numpy as jnp
from jax import lax
from jax.experimental import pallas as pl
from jax.experimental.pallas import tpu as pltpu
from jax.sharding import Mesh
from jax.sharding import PartitionSpec as P

NZ, NX = 8, 4
CHIPS = NZ * NX
HEADS, WIDTH = 24, 128
FIRST = 1
ROWS = HEADS // NX
MESH_IDS = pl.DeviceIdType.MESH


def chip(index):
    return {"sp_0": lax.div(index, NX), "sp_1": lax.rem(index, NX)}


def kernel(q_hbm, k_hbm, v_hbm, out_ref, raw, wide, stage, recv, far, outs,
           load_sem, send_sem, recv_sem, swap_send, swap_recv, back_send, back_recv):
    tokens = raw.shape[1]
    z, x, core = lax.axis_index("sp_0"), lax.axis_index("sp_1"), lax.axis_index("sp_2")
    me = z * NX + x
    head = (z - FIRST) * NX + x
    is_owner = (z >= FIRST) & (z < FIRST + ROWS)

    loads = [
        pltpu.make_async_copy(hbm, raw.at[t], load_sem.at[t])
        for t, hbm in enumerate((q_hbm, k_hbm, v_hbm))
    ]
    for load in loads:
        load.start()

    barrier = pltpu.get_barrier_semaphore()

    @pl.loop(1, CHIPS)
    def _(i):
        pl.semaphore_signal(barrier, inc=1, device_id=chip(lax.rem(me + i, CHIPS)), device_id_type=MESH_IDS)

    pl.semaphore_signal(barrier, inc=1, device_id={"sp_2": 1 - core}, device_id_type=MESH_IDS)

    for t in range(3):
        loads[t].wait()
        wide[t] = raw[t].astype(jnp.float32).reshape(tokens * HEADS, WIDTH)
        for h in range(HEADS):
            stage[h, t] = wide[t, pl.ds(h, tokens, stride=HEADS), :].astype(jnp.bfloat16)

    pl.semaphore_wait(barrier, CHIPS)

    def to_owner(i):
        row = lax.div(i, NX)
        row = jnp.where(z >= NZ // 2, row, ROWS - 1 - row)
        h = row * NX + lax.rem(x + 1 + i, NX)
        copy = pltpu.make_async_remote_copy(
            src_ref=stage.at[h], dst_ref=recv.at[me], send_sem=send_sem.at[h], recv_sem=recv_sem.at[me],
            device_id=chip(FIRST * NX + h), device_id_type=MESH_IDS,
        )
        return h, copy

    @pl.loop(0, HEADS)
    def _(i):
        h, copy = to_owner(i)

        @pl.when(FIRST * NX + h != me)
        def _():
            copy.start()

    def back(peer):
        return pltpu.make_async_remote_copy(
            src_ref=outs.at[peer],
            dst_ref=out_ref.at[:, pl.ds(pl.multiple_of(head * WIDTH, WIDTH), WIDTH)],
            send_sem=back_send.at[peer], recv_sem=back_recv.at[head],
            device_id=chip(peer), device_id_type=MESH_IDS,
        )

    def swap(row):
        chunk = pl.ds(row * NX, NX)
        return pltpu.make_async_remote_copy(
            src_ref=recv.at[chunk, pl.ds(1, 2)], dst_ref=far.at[chunk],
            send_sem=swap_send.at[row], recv_sem=swap_recv.at[row],
            device_id={"sp_2": 1 - core}, device_id_type=MESH_IDS,
        )

    @pl.when(is_owner)
    def _():
        recv[me] = stage[head]

        @pl.loop(0, NZ)
        def _(row):
            @pl.loop(0, NX)
            def _(j):
                source = row * NX + j

                @pl.when(source != me)
                def _():
                    pltpu.make_async_copy(recv.at[source], recv.at[source], recv_sem.at[source]).wait()

            swap(row).start()

        @pl.loop(0, NZ)
        def _(row):
            swap(row).wait_recv()

        factor = math.log2(math.e) / WIDTH**0.5
        dims = (((1,), (1,)), ((), ()))

        @pl.loop(0, NZ)
        def _(row):
            q = recv[pl.ds(row * NX, NX), 0].reshape(NX * tokens, WIDTH)
            k_near = recv[:, 1].reshape(CHIPS * tokens, WIDTH)
            k_far = far[:, 0].reshape(CHIPS * tokens, WIDTH)
            s_near = lax.dot_general(q, k_near, dims, preferred_element_type=jnp.float32)
            s_far = lax.dot_general(q, k_far, dims, preferred_element_type=jnp.float32)
            top = jnp.maximum(
                jnp.max(s_near, axis=1, keepdims=True), jnp.max(s_far, axis=1, keepdims=True)
            )
            p_near = jnp.exp2((s_near - top) * factor)
            p_far = jnp.exp2((s_far - top) * factor)
            total = jnp.sum(p_near, axis=1, keepdims=True) + jnp.sum(p_far, axis=1, keepdims=True)
            v_near = recv[:, 2].reshape(CHIPS * tokens, WIDTH)
            v_far = far[:, 1].reshape(CHIPS * tokens, WIDTH)
            acc = jnp.dot(p_near.astype(jnp.bfloat16), v_near, preferred_element_type=jnp.float32)
            acc += jnp.dot(p_far.astype(jnp.bfloat16), v_far, preferred_element_type=jnp.float32)
            result = (acc / total).astype(jnp.bfloat16)
            outs[pl.ds(row * NX, NX)] = result.reshape(NX, tokens, WIDTH)

            @pl.loop(0, NX)
            def _(j):
                peer = row * NX + j

                @pl.when(peer != me)
                def _():
                    back(peer).start()

                @pl.when(peer == me)
                def _():
                    out_ref[:, pl.ds(pl.multiple_of(head * WIDTH, WIDTH), WIDTH)] = outs[peer]

        @pl.loop(0, NZ)
        def _(row):
            swap(row).wait_send()

        @pl.loop(0, CHIPS)
        def _(peer):
            @pl.when(peer != me)
            def _():
                back(peer).wait_send()

    @pl.loop(0, HEADS)
    def _(h):
        @pl.when(FIRST * NX + h != me)
        def _():
            pltpu.make_async_copy(stage.at[h], stage.at[h], send_sem.at[h]).wait()
            pltpu.make_async_copy(outs.at[0], outs.at[0], back_recv.at[h]).wait()


def shards(queries, keys, values):
    tokens = queries.shape[0]
    dma = pltpu.SemaphoreType.DMA
    block = (tokens, WIDTH)
    return pl.pallas_call(
        kernel,
        out_shape=jax.ShapeDtypeStruct((tokens, HEADS * WIDTH), jnp.bfloat16),
        in_specs=[pl.BlockSpec(memory_space=pl.ANY)] * 3,
        out_specs=pl.BlockSpec(memory_space=pltpu.VMEM),
        scratch_shapes=[
            pltpu.VMEM((3, tokens, HEADS, WIDTH), jnp.bfloat16),
            pltpu.VMEM((3, tokens * HEADS, WIDTH), jnp.float32),
            pltpu.VMEM((HEADS, 3, *block), jnp.bfloat16),
            pltpu.VMEM((CHIPS, 3, *block), jnp.bfloat16),
            pltpu.VMEM((CHIPS, 2, *block), jnp.bfloat16),
            pltpu.VMEM((CHIPS, *block), jnp.bfloat16),
            dma((3,)),
            dma((HEADS,)),
            dma((CHIPS,)),
            dma((NZ,)),
            dma((NZ,)),
            dma((CHIPS,)),
            dma((HEADS,)),
        ],
        compiler_params=pltpu.CompilerParams(
            collective_id=0, has_side_effects=True, vmem_limit_bytes=48 * 1024 * 1024
        ),
    )(queries, keys, values)


def solution(mesh):
    finer = Mesh(mesh.devices.reshape(NZ, NX, 2, mesh.shape["dp"]), ("sp_0", "sp_1", "sp_2", "dp"))
    tokens = P(("dp", "sp_0", "sp_1", "sp_2"), None, None)
    return jax.shard_map(
        shards,
        mesh=finer,
        in_specs=(tokens,) * 3,
        out_specs=P(("dp", "sp_0", "sp_1", "sp_2"), None),
        check_vma=False,
    )
```

```python
import math

import jax
import jax.numpy as jnp
from jax import lax
from jax.experimental import pallas as pl
from jax.experimental.pallas import tpu as pltpu
from jax.sharding import Mesh
from jax.sharding import PartitionSpec as P

NZ, NX = 8, 4
CHIPS = NZ * NX
HEADS, WIDTH = 24, 128
FIRST = 1
ROWS = HEADS // NX
SKIP = FIRST * NX
MESH_IDS = pl.DeviceIdType.MESH


def kernel(q_hbm, k_hbm, v_hbm, out_ref, raw, wide, stage, stage_q, near, queries, far, outs,
           load_sem, kv_send, kv_recv, q_send, q_recv, swap_send, swap_recv, back_send, back_recv, ready):
    tokens = raw.shape[1]
    z, x, core = lax.axis_index("sp_0"), lax.axis_index("sp_1"), lax.axis_index("sp_2")
    me = z * NX + x
    head = me - SKIP
    is_owner = (z >= FIRST) & (z < FIRST + ROWS)

    loads = [
        pltpu.make_async_copy(hbm, raw.at[t], load_sem.at[t])
        for t, hbm in enumerate((k_hbm, v_hbm, q_hbm))
    ]
    for load in loads:
        load.start()

    barrier = pltpu.get_barrier_semaphore()

    def signal(semaphore, where):
        pl.semaphore_signal(semaphore, inc=1, device_id=where, device_id_type=MESH_IDS)

    def columns_of(body):
        for step in range(NX):
            to = x + step
            body(jnp.where(to >= NX, to - NX, to))

    @pl.when(is_owner)
    def _():
        signal(barrier, {"sp_2": 1 - core})

        @pl.loop(x + 1, NX)
        def _(to):
            signal(barrier, {"sp_1": to})

        @pl.loop(z + 1, NZ)
        def _(row):
            columns_of(lambda to: signal(barrier, {"sp_0": row, "sp_1": to}))

        columns_of(lambda to: signal(barrier, {"sp_0": 0, "sp_1": to}))

    def by_head(t, place):
        loads[t].wait()
        wide[t] = raw[t].astype(jnp.float32).reshape(tokens * HEADS, WIDTH)
        for h in range(HEADS):
            place(h, wide[t, pl.ds(h, tokens, stride=HEADS), :].astype(jnp.bfloat16))

    def place_kv(t):
        def place(h, block):
            stage[h, t] = block

        return place

    def place_q(h, block):
        stage_q[h] = block

    by_head(0, place_kv(0))
    by_head(1, place_kv(1))

    pl.semaphore_wait(barrier, jnp.where(is_owner, head + 1, HEADS))

    @pl.when(is_owner)
    def _():
        mine = ready.at[z - FIRST, x]

        @pl.loop(0, z - FIRST)
        def _(i):
            row = z - 1 - i
            columns_of(lambda to: signal(mine, {"sp_0": row, "sp_1": to}))

        @pl.loop(0, x)
        def _(to):
            signal(mine, {"sp_1": to})

    def kv_copy(row, to):
        h = (row - FIRST) * NX + to
        return pltpu.make_async_remote_copy(
            src_ref=stage.at[h], dst_ref=near.at[me], send_sem=kv_send.at[h], recv_sem=kv_recv.at[me],
            device_id={"sp_0": row, "sp_1": to}, device_id_type=MESH_IDS,
        )

    def q_copy(row, to):
        h = (row - FIRST) * NX + to
        return pltpu.make_async_remote_copy(
            src_ref=stage_q.at[h], dst_ref=queries.at[me], send_sem=q_send.at[h], recv_sem=q_recv.at[me],
            device_id={"sp_0": row, "sp_1": to}, device_id_type=MESH_IDS,
        )

    @pl.loop(FIRST, jnp.minimum(z, FIRST + ROWS))
    def _(row):
        columns_of(lambda to: kv_copy(row, to).start())

    @pl.when(is_owner)
    def _():
        @pl.loop(0, x)
        def _(to):
            kv_copy(z, to).start()

    by_head(2, place_q)

    @pl.when(is_owner)
    def _():
        @pl.loop(x + 1, NX)
        def _(to):
            pl.semaphore_wait(ready.at[z - FIRST, to], 1)
            kv_copy(z, to).start()

    @pl.loop(jnp.maximum(z + 1, FIRST), FIRST + ROWS)
    def _(row):
        def send(to):
            @pl.when(z > 0)
            def _():
                pl.semaphore_wait(ready.at[row - FIRST, to], 1)

            kv_copy(row, to).start()

        columns_of(send)

    @pl.loop(0, ROWS)
    def _(i):
        row = jnp.where(z < NZ // 2, FIRST + ROWS - 1 - i, FIRST + i)

        def send(to):
            @pl.when((row != z) | (to != x))
            def _():
                q_copy(row, to).start()

        columns_of(send)

    columns = pl.ds(pl.multiple_of(jnp.clip(head, 0, HEADS - 1) * WIDTH, WIDTH), WIDTH)

    def back(row, to):
        peer = row * NX + to
        return pltpu.make_async_remote_copy(
            src_ref=outs.at[peer], dst_ref=out_ref.at[:, columns],
            send_sem=back_send.at[peer], recv_sem=back_recv.at[head],
            device_id={"sp_0": row, "sp_1": to}, device_id_type=MESH_IDS,
        )

    def swap(row):
        chunk = pl.ds(row * NX, NX)
        return pltpu.make_async_remote_copy(
            src_ref=near.at[chunk], dst_ref=far.at[chunk],
            send_sem=swap_send.at[row], recv_sem=swap_recv.at[row],
            device_id={"sp_2": 1 - core}, device_id_type=MESH_IDS,
        )

    def of_row(row, body):
        def one(to):
            @pl.when((row != z) | (to != x))
            def _():
                body(row * NX + to)

        columns_of(one)

    def of_row_back(row, act):
        def one(to):
            @pl.when((row != z) | (to != x))
            def _():
                act(back(row, to))

        columns_of(one)

    @pl.when(is_owner)
    def _():
        near[me] = stage[head]
        queries[me] = stage_q[head]
        low = z < NZ // 2

        def nth_row(i):
            own = z + i
            own = jnp.where(own >= jnp.where(low, NZ // 2, NZ), own - NZ // 2, own)
            return jnp.where(i < NZ // 2, own, jnp.where(low, i, NZ - 1 - i))

        @pl.loop(0, NZ)
        def _(i):
            row = nth_row(i)
            of_row(row, lambda s: pltpu.make_async_copy(near.at[s], near.at[s], kv_recv.at[s]).wait())
            swap(row).start()

        @pl.loop(0, NZ)
        def _(row):
            swap(row).wait_recv()

        factor = math.log2(math.e) / WIDTH**0.5
        dims = (((1,), (1,)), ((), ()))

        @pl.loop(0, NZ)
        def _(i):
            row = nth_row(i)
            of_row(row, lambda s: pltpu.make_async_copy(queries.at[s], queries.at[s], q_recv.at[s]).wait())
            q = queries[pl.ds(row * NX, NX)].reshape(NX * tokens, WIDTH)
            k_near = near[:, 0].reshape(CHIPS * tokens, WIDTH)
            k_far = far[:, 0].reshape(CHIPS * tokens, WIDTH)
            s_near = lax.dot_general(q, k_near, dims, preferred_element_type=jnp.float32)
            s_far = lax.dot_general(q, k_far, dims, preferred_element_type=jnp.float32)
            top = jnp.maximum(
                jnp.max(s_near, axis=1, keepdims=True), jnp.max(s_far, axis=1, keepdims=True)
            )
            p_near = jnp.exp2((s_near - top) * factor)
            p_far = jnp.exp2((s_far - top) * factor)
            total = jnp.sum(p_near, axis=1, keepdims=True) + jnp.sum(p_far, axis=1, keepdims=True)
            v_near = near[:, 1].reshape(CHIPS * tokens, WIDTH)
            v_far = far[:, 1].reshape(CHIPS * tokens, WIDTH)
            acc = jnp.dot(p_near.astype(jnp.bfloat16), v_near, preferred_element_type=jnp.float32)
            acc += jnp.dot(p_far.astype(jnp.bfloat16), v_far, preferred_element_type=jnp.float32)
            result = (acc / total).astype(jnp.bfloat16)
            outs[pl.ds(row * NX, NX)] = result.reshape(NX, tokens, WIDTH)
            of_row_back(row, lambda copy: copy.start())

        out_ref[:, columns] = outs[me]

        @pl.loop(0, NZ)
        def _(row):
            swap(row).wait_send()
            of_row_back(row, lambda copy: copy.wait_send())

    @pl.loop(0, HEADS)
    def _(h):
        @pl.when(h != head)
        def _():
            pltpu.make_async_copy(stage.at[h], stage.at[h], kv_send.at[h]).wait()
            pltpu.make_async_copy(stage_q.at[h], stage_q.at[h], q_send.at[h]).wait()
            pltpu.make_async_copy(outs.at[0], outs.at[0], back_recv.at[h]).wait()


def shards(queries, keys, values):
    tokens = queries.shape[0]
    dma = pltpu.SemaphoreType.DMA
    bf16 = jnp.bfloat16
    block = (tokens, WIDTH)
    return pl.pallas_call(
        kernel,
        out_shape=jax.ShapeDtypeStruct((tokens, HEADS * WIDTH), bf16),
        in_specs=[pl.BlockSpec(memory_space=pl.ANY)] * 3,
        out_specs=pl.BlockSpec(memory_space=pltpu.VMEM),
        scratch_shapes=[
            pltpu.VMEM((3, tokens, HEADS, WIDTH), bf16),
            pltpu.VMEM((3, tokens * HEADS, WIDTH), jnp.float32),
            pltpu.VMEM((HEADS, 2, *block), bf16),
            pltpu.VMEM((HEADS, *block), bf16),
            pltpu.VMEM((CHIPS, 2, *block), bf16),
            pltpu.VMEM((CHIPS, *block), bf16),
            pltpu.VMEM((CHIPS, 2, *block), bf16),
            pltpu.VMEM((CHIPS, *block), bf16),
            dma((3,)),
            dma((HEADS,)),
            dma((CHIPS,)),
            dma((HEADS,)),
            dma((CHIPS,)),
            dma((NZ,)),
            dma((NZ,)),
            dma((CHIPS,)),
            dma((HEADS,)),
            pltpu.SemaphoreType.REGULAR((ROWS, NX)),
        ],
        compiler_params=pltpu.CompilerParams(
            collective_id=0, has_side_effects=True, vmem_limit_bytes=54800 * 1024
        ),
    )(queries, keys, values)


def solution(mesh):
    finer = Mesh(mesh.devices.reshape(NZ, NX, 2, mesh.shape["dp"]), ("sp_0", "sp_1", "sp_2", "dp"))
    tokens = P(("dp", "sp_0", "sp_1", "sp_2"), None, None)
    return jax.shard_map(
        shards,
        mesh=finer,
        in_specs=(tokens,) * 3,
        out_specs=P(("dp", "sp_0", "sp_1", "sp_2"), None),
        check_vma=False,
    )
```

```python
import math

import jax
import jax.numpy as jnp
from jax import lax
from jax.experimental import pallas as pl
from jax.experimental.pallas import tpu as pltpu
from jax.sharding import Mesh
from jax.sharding import PartitionSpec as P

NZ, NX = 8, 4
CHIPS = NZ * NX
HEADS, WIDTH = 24, 128
FIRST = 1
ROWS = HEADS // NX
SKIP = FIRST * NX
MESH_IDS = pl.DeviceIdType.MESH


def kernel(q_hbm, k_hbm, v_hbm, out_ref, raw, wide, stage, stage_q, near, queries, far, outs,
           load_sem, kv_send, kv_recv, q_send, q_recv, swap_send, swap_recv, back_send, back_recv, ready):
    tokens = raw.shape[1]
    z, x, core = lax.axis_index("sp_0"), lax.axis_index("sp_1"), lax.axis_index("sp_2")
    me = z * NX + x
    head = me - SKIP
    is_owner = (z >= FIRST) & (z < FIRST + ROWS)

    loads = [
        pltpu.make_async_copy(hbm, raw.at[t], load_sem.at[t])
        for t, hbm in enumerate((k_hbm, v_hbm, q_hbm))
    ]
    for load in loads:
        load.start()

    barrier = pltpu.get_barrier_semaphore()

    def signal(semaphore, where):
        pl.semaphore_signal(semaphore, inc=1, device_id=where, device_id_type=MESH_IDS)

    def columns_of(body):
        for step in range(NX):
            to = x + step
            body(jnp.where(to >= NX, to - NX, to))

    @pl.when(is_owner)
    def _():
        signal(barrier, {"sp_2": 1 - core})

        @pl.loop(x + 1, NX)
        def _(to):
            signal(barrier, {"sp_1": to})

        @pl.loop(z + 1, NZ)
        def _(row):
            columns_of(lambda to: signal(barrier, {"sp_0": row, "sp_1": to}))

        columns_of(lambda to: signal(barrier, {"sp_0": 0, "sp_1": to}))

    def by_head(t, place):
        loads[t].wait()
        wide[t] = raw[t].astype(jnp.float32).reshape(tokens * HEADS, WIDTH)
        for h in range(HEADS):
            place(h, wide[t, pl.ds(h, tokens, stride=HEADS), :].astype(jnp.bfloat16))

    def place_kv(t):
        def place(h, block):
            stage[h, t] = block

        return place

    def place_q(h, block):
        stage_q[h] = block

    pl.semaphore_wait(barrier, jnp.where(is_owner, head + 1, HEADS))

    @pl.when(is_owner)
    def _():
        mine = ready.at[z - FIRST, x]

        @pl.loop(0, z - FIRST)
        def _(i):
            row = z - 1 - i
            columns_of(lambda to: signal(mine, {"sp_0": row, "sp_1": to}))

        @pl.loop(0, x)
        def _(to):
            signal(mine, {"sp_1": to})

    by_head(0, place_kv(0))
    by_head(1, place_kv(1))

    def kv_copy(row, to):
        h = (row - FIRST) * NX + to
        return pltpu.make_async_remote_copy(
            src_ref=stage.at[h], dst_ref=near.at[me], send_sem=kv_send.at[h], recv_sem=kv_recv.at[me],
            device_id={"sp_0": row, "sp_1": to}, device_id_type=MESH_IDS,
        )

    def q_copy(row, to):
        h = (row - FIRST) * NX + to
        return pltpu.make_async_remote_copy(
            src_ref=stage_q.at[h], dst_ref=queries.at[me], send_sem=q_send.at[h], recv_sem=q_recv.at[me],
            device_id={"sp_0": row, "sp_1": to}, device_id_type=MESH_IDS,
        )

    by_head(2, place_q)

    def kv_row(row):
        def send(to):
            @pl.when(is_owner & ((row > z) | ((row == z) & (to > x))))
            def _():
                pl.semaphore_wait(ready.at[row - FIRST, to], 1)

            @pl.when((row != z) | (to != x))
            def _():
                kv_copy(row, to).start()

        columns_of(send)

    def q_row(row):
        def send(to):
            @pl.when((row != z) | (to != x))
            def _():
                q_copy(row, to).start()

        columns_of(send)

    for send_row, i in ((kv_row, 0), (kv_row, 1), (kv_row, 2), (q_row, 0), (q_row, 1), (q_row, 2)):
        send_row(NZ // 2 - 1 - i)
        send_row(NZ // 2 + i)

    columns = pl.ds(pl.multiple_of(jnp.clip(head, 0, HEADS - 1) * WIDTH, WIDTH), WIDTH)

    def back(row, to):
        peer = row * NX + to
        return pltpu.make_async_remote_copy(
            src_ref=outs.at[peer], dst_ref=out_ref.at[:, columns],
            send_sem=back_send.at[peer], recv_sem=back_recv.at[head],
            device_id={"sp_0": row, "sp_1": to}, device_id_type=MESH_IDS,
        )

    def swap(row):
        chunk = pl.ds(row * NX, NX)
        return pltpu.make_async_remote_copy(
            src_ref=near.at[chunk], dst_ref=far.at[chunk],
            send_sem=swap_send.at[row], recv_sem=swap_recv.at[row],
            device_id={"sp_2": 1 - core}, device_id_type=MESH_IDS,
        )

    def of_row(row, body):
        def one(to):
            @pl.when((row != z) | (to != x))
            def _():
                body(row * NX + to)

        columns_of(one)

    def of_row_back(row, act):
        def one(to):
            @pl.when((row != z) | (to != x))
            def _():
                act(back(row, to))

        columns_of(one)

    @pl.when(is_owner)
    def _():
        near[me] = stage[head]
        queries[me] = stage_q[head]
        low = z < NZ // 2

        def nth_row(i):
            own = z + i - NZ // 2
            own = jnp.where(own >= jnp.where(low, NZ // 2, NZ), own - NZ // 2, own)
            cross = jnp.where(low, NZ // 2 + i, NZ // 2 - 1 - i)
            return jnp.where(i < NZ // 2, cross, own)

        @pl.loop(0, NZ)
        def _(i):
            row = nth_row(i)
            of_row(row, lambda s: pltpu.make_async_copy(near.at[s], near.at[s], kv_recv.at[s]).wait())
            swap(row).start()

        @pl.loop(0, NZ)
        def _(row):
            swap(row).wait_recv()

        factor = math.log2(math.e) / WIDTH**0.5
        dims = (((1,), (1,)), ((), ()))

        @pl.loop(0, NZ)
        def _(i):
            row = nth_row(i)
            of_row(row, lambda s: pltpu.make_async_copy(queries.at[s], queries.at[s], q_recv.at[s]).wait())
            q = queries[pl.ds(row * NX, NX)].reshape(NX * tokens, WIDTH)
            k_near = near[:, 0].reshape(CHIPS * tokens, WIDTH)
            k_far = far[:, 0].reshape(CHIPS * tokens, WIDTH)
            s_near = lax.dot_general(q, k_near, dims, preferred_element_type=jnp.float32)
            s_far = lax.dot_general(q, k_far, dims, preferred_element_type=jnp.float32)
            top = jnp.maximum(
                jnp.max(s_near, axis=1, keepdims=True), jnp.max(s_far, axis=1, keepdims=True)
            )
            p_near = jnp.exp2((s_near - top) * factor)
            p_far = jnp.exp2((s_far - top) * factor)
            total = jnp.sum(p_near, axis=1, keepdims=True) + jnp.sum(p_far, axis=1, keepdims=True)
            v_near = near[:, 1].reshape(CHIPS * tokens, WIDTH)
            v_far = far[:, 1].reshape(CHIPS * tokens, WIDTH)
            acc = jnp.dot(p_near.astype(jnp.bfloat16), v_near, preferred_element_type=jnp.float32)
            acc += jnp.dot(p_far.astype(jnp.bfloat16), v_far, preferred_element_type=jnp.float32)
            result = (acc / total).astype(jnp.bfloat16)
            outs[pl.ds(row * NX, NX)] = result.reshape(NX, tokens, WIDTH)
            of_row_back(row, lambda copy: copy.start())

        out_ref[:, columns] = outs[me]

        @pl.loop(0, NZ)
        def _(row):
            swap(row).wait_send()
            of_row_back(row, lambda copy: copy.wait_send())

    @pl.loop(0, HEADS)
    def _(h):
        @pl.when(h != head)
        def _():
            pltpu.make_async_copy(stage.at[h], stage.at[h], kv_send.at[h]).wait()
            pltpu.make_async_copy(stage_q.at[h], stage_q.at[h], q_send.at[h]).wait()
            pltpu.make_async_copy(outs.at[0], outs.at[0], back_recv.at[h]).wait()


def shards(queries, keys, values):
    tokens = queries.shape[0]
    dma = pltpu.SemaphoreType.DMA
    bf16 = jnp.bfloat16
    block = (tokens, WIDTH)
    return pl.pallas_call(
        kernel,
        out_shape=jax.ShapeDtypeStruct((tokens, HEADS * WIDTH), bf16),
        in_specs=[pl.BlockSpec(memory_space=pl.ANY)] * 3,
        out_specs=pl.BlockSpec(memory_space=pltpu.VMEM),
        scratch_shapes=[
            pltpu.VMEM((3, tokens, HEADS, WIDTH), bf16),
            pltpu.VMEM((3, tokens * HEADS, WIDTH), jnp.float32),
            pltpu.VMEM((HEADS, 2, *block), bf16),
            pltpu.VMEM((HEADS, *block), bf16),
            pltpu.VMEM((CHIPS, 2, *block), bf16),
            pltpu.VMEM((CHIPS, *block), bf16),
            pltpu.VMEM((CHIPS, 2, *block), bf16),
            pltpu.VMEM((CHIPS, *block), bf16),
            dma((3,)),
            dma((HEADS,)),
            dma((CHIPS,)),
            dma((HEADS,)),
            dma((CHIPS,)),
            dma((NZ,)),
            dma((NZ,)),
            dma((CHIPS,)),
            dma((HEADS,)),
            pltpu.SemaphoreType.REGULAR((ROWS, NX)),
        ],
        compiler_params=pltpu.CompilerParams(
            collective_id=0, has_side_effects=True, vmem_limit_bytes=54800 * 1024
        ),
    )(queries, keys, values)


def solution(mesh):
    finer = Mesh(mesh.devices.reshape(NZ, NX, 2, mesh.shape["dp"]), ("sp_0", "sp_1", "sp_2", "dp"))
    tokens = P(("dp", "sp_0", "sp_1", "sp_2"), None, None)
    return jax.shard_map(
        shards,
        mesh=finer,
        in_specs=(tokens,) * 3,
        out_specs=P(("dp", "sp_0", "sp_1", "sp_2"), None),
        check_vma=False,
    )
```

```python
import math

import jax
import jax.numpy as jnp
from jax import lax
from jax.experimental import pallas as pl
from jax.experimental.pallas import tpu as pltpu
from jax.sharding import Mesh
from jax.sharding import PartitionSpec as P

NZ, NX = 8, 4
CHIPS = NZ * NX
HEADS, WIDTH = 24, 128
FIRST = 1
ROWS = HEADS // NX
SKIP = FIRST * NX
MESH_IDS = pl.DeviceIdType.MESH


def kernel(q_hbm, k_hbm, v_hbm, out_ref, raw, wide, stage, stage_q, near, queries, far, outs,
           load_sem, kv_send, kv_recv, q_send, q_recv, swap_send, swap_recv, back_send, back_recv, ready):
    tokens = raw.shape[1]
    z, x, core = lax.axis_index("sp_0"), lax.axis_index("sp_1"), lax.axis_index("sp_2")
    me = z * NX + x
    head = me - SKIP
    is_owner = (z >= FIRST) & (z < FIRST + ROWS)

    loads = [
        pltpu.make_async_copy(hbm, raw.at[t], load_sem.at[t])
        for t, hbm in enumerate((k_hbm, v_hbm, q_hbm))
    ]
    for load in loads:
        load.start()

    barrier = pltpu.get_barrier_semaphore()

    def signal(semaphore, where):
        pl.semaphore_signal(semaphore, inc=1, device_id=where, device_id_type=MESH_IDS)

    def columns_of(body):
        for step in range(NX):
            to = x + step
            body(jnp.where(to >= NX, to - NX, to))

    @pl.when(is_owner)
    def _():
        signal(barrier, {"sp_2": 1 - core})

        @pl.loop(x + 1, NX)
        def _(to):
            signal(barrier, {"sp_1": to})

        @pl.loop(z + 1, NZ)
        def _(row):
            columns_of(lambda to: signal(barrier, {"sp_0": row, "sp_1": to}))

        columns_of(lambda to: signal(barrier, {"sp_0": 0, "sp_1": to}))

    def by_head(t, place):
        loads[t].wait()
        wide[t] = raw[t].astype(jnp.float32).reshape(tokens * HEADS, WIDTH)
        for h in range(HEADS):
            place(h, wide[t, pl.ds(h, tokens, stride=HEADS), :].astype(jnp.bfloat16))

    def place_kv(t):
        def place(h, block):
            stage[h, t] = block

        return place

    def place_q(h, block):
        stage_q[h] = block

    pl.semaphore_wait(barrier, jnp.where(is_owner, head + 1, HEADS))

    @pl.when(is_owner)
    def _():
        mine = ready.at[z - FIRST, x]

        @pl.loop(0, z - FIRST)
        def _(i):
            row = z - 1 - i
            columns_of(lambda to: signal(mine, {"sp_0": row, "sp_1": to}))

        @pl.loop(0, x)
        def _(to):
            signal(mine, {"sp_1": to})

    by_head(0, place_kv(0))
    by_head(1, place_kv(1))

    def kv_copy(row, to):
        h = (row - FIRST) * NX + to
        return pltpu.make_async_remote_copy(
            src_ref=stage.at[h], dst_ref=near.at[me], send_sem=kv_send.at[h], recv_sem=kv_recv.at[me],
            device_id={"sp_0": row, "sp_1": to}, device_id_type=MESH_IDS,
        )

    def q_copy(row, to):
        h = (row - FIRST) * NX + to
        return pltpu.make_async_remote_copy(
            src_ref=stage_q.at[h], dst_ref=queries.at[me], send_sem=q_send.at[h], recv_sem=q_recv.at[me],
            device_id={"sp_0": row, "sp_1": to}, device_id_type=MESH_IDS,
        )

    def kv_row(row):
        def send(to):
            @pl.when(is_owner & ((row > z) | ((row == z) & (to > x))))
            def _():
                pl.semaphore_wait(ready.at[row - FIRST, to], 1)

            @pl.when((row != z) | (to != x))
            def _():
                kv_copy(row, to).start()

        columns_of(send)

    def q_row(row):
        def send(to):
            @pl.when((row != z) | (to != x))
            def _():
                q_copy(row, to).start()

        columns_of(send)

    for i in range(ROWS // 2):
        kv_row(NZ // 2 - 1 - i)
        kv_row(NZ // 2 + i)

    by_head(2, place_q)

    for i in range(ROWS // 2):
        q_row(NZ // 2 - 1 - i)
        q_row(NZ // 2 + i)

    columns = pl.ds(pl.multiple_of(jnp.clip(head, 0, HEADS - 1) * WIDTH, WIDTH), WIDTH)

    def back(row, to):
        peer = row * NX + to
        return pltpu.make_async_remote_copy(
            src_ref=outs.at[peer], dst_ref=out_ref.at[:, columns],
            send_sem=back_send.at[peer], recv_sem=back_recv.at[head],
            device_id={"sp_0": row, "sp_1": to}, device_id_type=MESH_IDS,
        )

    def swap(row):
        chunk = pl.ds(row * NX, NX)
        return pltpu.make_async_remote_copy(
            src_ref=near.at[chunk], dst_ref=far.at[chunk],
            send_sem=swap_send.at[row], recv_sem=swap_recv.at[row],
            device_id={"sp_2": 1 - core}, device_id_type=MESH_IDS,
        )

    def of_row(row, body):
        def one(to):
            @pl.when((row != z) | (to != x))
            def _():
                body(row * NX + to)

        columns_of(one)

    def of_row_back(row, act):
        def one(to):
            @pl.when((row != z) | (to != x))
            def _():
                act(back(row, to))

        columns_of(one)

    @pl.when(is_owner)
    def _():
        near[me] = stage[head]
        queries[me] = stage_q[head]
        low = z < NZ // 2

        def nth_row(i):
            own = z + i - NZ // 2
            own = jnp.where(own >= jnp.where(low, NZ // 2, NZ), own - NZ // 2, own)
            cross = jnp.where(low, NZ // 2 + i, NZ // 2 - 1 - i)
            return jnp.where(i < NZ // 2, cross, own)

        @pl.loop(0, NZ)
        def _(i):
            row = nth_row(i)
            of_row(row, lambda s: pltpu.make_async_copy(near.at[s], near.at[s], kv_recv.at[s]).wait())
            swap(row).start()

        factor = math.log2(math.e) / WIDTH**0.5
        dims = (((1,), (1,)), ((), ()))

        def attend(i, first=False):
            own = jnp.where(low, 0, NZ // 2) + 2 * i - NZ // 2
            cross = jnp.where(low, NZ - 2 - 2 * i, 2 * i)
            row = jnp.where(i < NZ // 4, cross, own)
            for r in range(2):
                of_row(row + r, lambda s: pltpu.make_async_copy(queries.at[s], queries.at[s], q_recv.at[s]).wait())
            q = queries[pl.ds(row * NX, 2 * NX)].reshape(2 * NX * tokens, WIDTH)

            def half(part):
                k = part[:, 0].reshape(CHIPS * tokens, WIDTH)
                v = part[:, 1].reshape(CHIPS * tokens, WIDTH)
                scores = lax.dot_general(q, k, dims, preferred_element_type=jnp.float32)
                return scores, v

            scores, v = half(near)
            top_near = jnp.max(scores, axis=1, keepdims=True)
            p = jnp.exp2((scores - top_near) * factor)
            total = jnp.sum(p, axis=1, keepdims=True)
            acc = jnp.dot(p.astype(jnp.bfloat16), v, preferred_element_type=jnp.float32)
            if first:

                @pl.loop(0, NZ)
                def _(row):
                    swap(row).wait_recv()

            scores, v = half(far)
            top = jnp.maximum(top_near, jnp.max(scores, axis=1, keepdims=True))
            p = jnp.exp2((scores - top) * factor)
            shrink = jnp.exp2((top_near - top) * factor)
            total = total * shrink + jnp.sum(p, axis=1, keepdims=True)
            acc = acc * shrink + jnp.dot(p.astype(jnp.bfloat16), v, preferred_element_type=jnp.float32)
            result = (acc / total).astype(jnp.bfloat16)
            outs[pl.ds(row * NX, 2 * NX)] = result.reshape(2 * NX, tokens, WIDTH)
            for r in range(2):
                of_row_back(row + r, lambda copy: copy.start())

        attend(0, first=True)
        pl.loop(1, NZ // 2)(attend)
        out_ref[:, columns] = outs[me]

        @pl.loop(0, NZ)
        def _(row):
            swap(row).wait_send()
            of_row_back(row, lambda copy: copy.wait_send())

    @pl.loop(0, HEADS)
    def _(h):
        @pl.when(h != head)
        def _():
            pltpu.make_async_copy(stage.at[h], stage.at[h], kv_send.at[h]).wait()
            pltpu.make_async_copy(stage_q.at[h], stage_q.at[h], q_send.at[h]).wait()
            pltpu.make_async_copy(outs.at[0], outs.at[0], back_recv.at[h]).wait()


def shards(queries, keys, values):
    tokens = queries.shape[0]
    dma = pltpu.SemaphoreType.DMA
    bf16 = jnp.bfloat16
    block = (tokens, WIDTH)
    return pl.pallas_call(
        kernel,
        out_shape=jax.ShapeDtypeStruct((tokens, HEADS * WIDTH), bf16),
        in_specs=[pl.BlockSpec(memory_space=pl.ANY)] * 3,
        out_specs=pl.BlockSpec(memory_space=pltpu.VMEM),
        scratch_shapes=[
            pltpu.VMEM((3, tokens, HEADS, WIDTH), bf16),
            pltpu.VMEM((3, tokens * HEADS, WIDTH), jnp.float32),
            pltpu.VMEM((HEADS, 2, *block), bf16),
            pltpu.VMEM((HEADS, *block), bf16),
            pltpu.VMEM((CHIPS, 2, *block), bf16),
            pltpu.VMEM((CHIPS, *block), bf16),
            pltpu.VMEM((CHIPS, 2, *block), bf16),
            pltpu.VMEM((CHIPS, *block), bf16),
            dma((3,)),
            dma((HEADS,)),
            dma((CHIPS,)),
            dma((HEADS,)),
            dma((CHIPS,)),
            dma((NZ,)),
            dma((NZ,)),
            dma((CHIPS,)),
            dma((HEADS,)),
            pltpu.SemaphoreType.REGULAR((ROWS, NX)),
        ],
        compiler_params=pltpu.CompilerParams(
            collective_id=0, has_side_effects=True, vmem_limit_bytes=54800 * 1024
        ),
    )(queries, keys, values)


def solution(mesh):
    finer = Mesh(mesh.devices.reshape(NZ, NX, 2, mesh.shape["dp"]), ("sp_0", "sp_1", "sp_2", "dp"))
    tokens = P(("dp", "sp_0", "sp_1", "sp_2"), None, None)
    return jax.shard_map(
        shards,
        mesh=finer,
        in_specs=(tokens,) * 3,
        out_specs=P(("dp", "sp_0", "sp_1", "sp_2"), None),
        check_vma=False,
    )
```

```python
import math

import jax
import jax.numpy as jnp
from jax import lax
from jax.experimental import pallas as pl
from jax.experimental.pallas import tpu as pltpu
from jax.sharding import Mesh
from jax.sharding import PartitionSpec as P

NZ, NX = 8, 4
CHIPS = NZ * NX
HEADS, WIDTH = 24, 128
FIRST = 1
ROWS = HEADS // NX
SKIP = FIRST * NX
MESH_IDS = pl.DeviceIdType.MESH


def kernel(q_hbm, k_hbm, v_hbm, out_ref, raw, wide, stage, stage_q, near, queries, far, outs,
           load_sem, kv_send, kv_recv, q_send, q_recv, swap_send, swap_recv, back_send, back_recv, ready):
    tokens = raw.shape[1]
    z, x, core = lax.axis_index("sp_0"), lax.axis_index("sp_1"), lax.axis_index("sp_2")
    me = z * NX + x
    head = me - SKIP
    is_owner = (z >= FIRST) & (z < FIRST + ROWS)

    loads = [
        pltpu.make_async_copy(hbm, raw.at[t], load_sem.at[t])
        for t, hbm in enumerate((k_hbm, v_hbm, q_hbm))
    ]
    for load in loads:
        load.start()

    barrier = pltpu.get_barrier_semaphore()

    def signal(semaphore, where):
        pl.semaphore_signal(semaphore, inc=1, device_id=where, device_id_type=MESH_IDS)

    def columns_of(body):
        for step in range(NX):
            to = x + step
            body(jnp.where(to >= NX, to - NX, to))

    @pl.when(is_owner)
    def _():
        signal(barrier, {"sp_2": 1 - core})

        @pl.loop(x + 1, NX)
        def _(to):
            signal(barrier, {"sp_1": to})

        @pl.loop(z + 1, NZ)
        def _(row):
            columns_of(lambda to: signal(barrier, {"sp_0": row, "sp_1": to}))

        columns_of(lambda to: signal(barrier, {"sp_0": 0, "sp_1": to}))

    def by_head(t, place):
        loads[t].wait()
        wide[t] = raw[t].astype(jnp.float32).reshape(tokens * HEADS, WIDTH)
        for h in range(HEADS):
            place(h, wide[t, pl.ds(h, tokens, stride=HEADS), :].astype(jnp.bfloat16))

    def place_kv(t):
        def place(h, block):
            stage[h, t] = block

        return place

    def place_q(h, block):
        stage_q[h] = block

    pl.semaphore_wait(barrier, jnp.where(is_owner, head + 1, HEADS))

    @pl.when(is_owner)
    def _():
        mine = ready.at[z - FIRST, x]

        @pl.loop(0, z - FIRST)
        def _(i):
            row = z - 1 - i
            columns_of(lambda to: signal(mine, {"sp_0": row, "sp_1": to}))

        @pl.loop(0, x)
        def _(to):
            signal(mine, {"sp_1": to})

    by_head(0, place_kv(0))
    by_head(1, place_kv(1))

    def kv_copy(row, to):
        h = (row - FIRST) * NX + to
        return pltpu.make_async_remote_copy(
            src_ref=stage.at[h], dst_ref=near.at[me], send_sem=kv_send.at[h], recv_sem=kv_recv.at[me],
            device_id={"sp_0": row, "sp_1": to}, device_id_type=MESH_IDS,
        )

    def q_copy(row, to):
        h = (row - FIRST) * NX + to
        return pltpu.make_async_remote_copy(
            src_ref=stage_q.at[h], dst_ref=queries.at[me], send_sem=q_send.at[h], recv_sem=q_recv.at[me],
            device_id={"sp_0": row, "sp_1": to}, device_id_type=MESH_IDS,
        )

    def kv_row(row):
        def send(to):
            @pl.when(is_owner & ((row > z) | ((row == z) & (to > x))))
            def _():
                pl.semaphore_wait(ready.at[row - FIRST, to], 1)

            @pl.when((row != z) | (to != x))
            def _():
                kv_copy(row, to).start()

        columns_of(send)

    def q_row(row):
        def send(to):
            @pl.when((row != z) | (to != x))
            def _():
                q_copy(row, to).start()

        columns_of(send)

    for i in range(ROWS // 2):
        kv_row(NZ // 2 + i)
        kv_row(NZ // 2 - 1 - i)

    by_head(2, place_q)

    upper = z >= NZ // 2
    for i in range(ROWS):
        j = i % (ROWS // 2)
        q_row(jnp.where(upper == (i < ROWS // 2), NZ // 2 - 1 - j, NZ // 2 + j))

    columns = pl.ds(pl.multiple_of(jnp.clip(head, 0, HEADS - 1) * WIDTH, WIDTH), WIDTH)

    def back(row, to):
        peer = row * NX + to
        return pltpu.make_async_remote_copy(
            src_ref=outs.at[peer], dst_ref=out_ref.at[:, columns],
            send_sem=back_send.at[peer], recv_sem=back_recv.at[head],
            device_id={"sp_0": row, "sp_1": to}, device_id_type=MESH_IDS,
        )

    def swap(row):
        chunk = pl.ds(row * NX, NX)
        return pltpu.make_async_remote_copy(
            src_ref=near.at[chunk], dst_ref=far.at[chunk],
            send_sem=swap_send.at[row], recv_sem=swap_recv.at[row],
            device_id={"sp_2": 1 - core}, device_id_type=MESH_IDS,
        )

    def of_row(row, body):
        def one(to):
            @pl.when((row != z) | (to != x))
            def _():
                body(row * NX + to)

        columns_of(one)

    def of_row_back(row, act):
        def one(to):
            @pl.when((row != z) | (to != x))
            def _():
                act(back(row, to))

        columns_of(one)

    @pl.when(is_owner)
    def _():
        near[me] = stage[head]
        queries[me] = stage_q[head]
        low = z < NZ // 2

        def nth_row(i):
            own = z + i - NZ // 2
            own = jnp.where(own >= jnp.where(low, NZ // 2, NZ), own - NZ // 2, own)
            cross = jnp.where(low, NZ // 2 + i, NZ // 2 - 1 - i)
            return jnp.where(i < NZ // 2, cross, own)

        @pl.loop(0, NZ)
        def _(i):
            row = nth_row(i)
            of_row(row, lambda s: pltpu.make_async_copy(near.at[s], near.at[s], kv_recv.at[s]).wait())
            swap(row).start()

        factor = math.log2(math.e) / WIDTH**0.5
        dims = (((1,), (1,)), ((), ()))

        def attend(i, first=False):
            own = jnp.where(low, 0, NZ // 2) + 2 * i - NZ // 2
            cross = jnp.where(low, NZ - 2 - 2 * i, 2 * i)
            row = jnp.where(i < NZ // 4, cross, own)
            for r in range(2):
                of_row(row + r, lambda s: pltpu.make_async_copy(queries.at[s], queries.at[s], q_recv.at[s]).wait())
            q = queries[pl.ds(row * NX, 2 * NX)].reshape(2 * NX * tokens, WIDTH)

            def half(part):
                k = part[:, 0].reshape(CHIPS * tokens, WIDTH)
                v = part[:, 1].reshape(CHIPS * tokens, WIDTH)
                scores = lax.dot_general(q, k, dims, preferred_element_type=jnp.float32)
                return scores, v

            scores, v = half(near)
            top_near = jnp.max(scores, axis=1, keepdims=True)
            p = jnp.exp2((scores - top_near) * factor)
            total = jnp.sum(p, axis=1, keepdims=True)
            acc = jnp.dot(p.astype(jnp.bfloat16), v, preferred_element_type=jnp.float32)
            if first:

                @pl.loop(0, NZ)
                def _(row):
                    swap(row).wait_recv()

            scores, v = half(far)
            top = jnp.maximum(top_near, jnp.max(scores, axis=1, keepdims=True))
            p = jnp.exp2((scores - top) * factor)
            shrink = jnp.exp2((top_near - top) * factor)
            total = total * shrink + jnp.sum(p, axis=1, keepdims=True)
            acc = acc * shrink + jnp.dot(p.astype(jnp.bfloat16), v, preferred_element_type=jnp.float32)
            result = (acc / total).astype(jnp.bfloat16)
            outs[pl.ds(row * NX, 2 * NX)] = result.reshape(2 * NX, tokens, WIDTH)
            for r in range(2):
                of_row_back(row + r, lambda copy: copy.start())

        attend(0, first=True)
        pl.loop(1, NZ // 2)(attend)
        out_ref[:, columns] = outs[me]

        @pl.loop(0, NZ)
        def _(row):
            swap(row).wait_send()
            of_row_back(row, lambda copy: copy.wait_send())

    @pl.loop(0, HEADS)
    def _(h):
        @pl.when(h != head)
        def _():
            pltpu.make_async_copy(stage.at[h], stage.at[h], kv_send.at[h]).wait()
            pltpu.make_async_copy(stage_q.at[h], stage_q.at[h], q_send.at[h]).wait()
            pltpu.make_async_copy(outs.at[0], outs.at[0], back_recv.at[h]).wait()


def shards(queries, keys, values):
    tokens = queries.shape[0]
    dma = pltpu.SemaphoreType.DMA
    bf16 = jnp.bfloat16
    block = (tokens, WIDTH)
    return pl.pallas_call(
        kernel,
        out_shape=jax.ShapeDtypeStruct((tokens, HEADS * WIDTH), bf16),
        in_specs=[pl.BlockSpec(memory_space=pl.ANY)] * 3,
        out_specs=pl.BlockSpec(memory_space=pltpu.VMEM),
        scratch_shapes=[
            pltpu.VMEM((3, tokens, HEADS, WIDTH), bf16),
            pltpu.VMEM((3, tokens * HEADS, WIDTH), jnp.float32),
            pltpu.VMEM((HEADS, 2, *block), bf16),
            pltpu.VMEM((HEADS, *block), bf16),
            pltpu.VMEM((CHIPS, 2, *block), bf16),
            pltpu.VMEM((CHIPS, *block), bf16),
            pltpu.VMEM((CHIPS, 2, *block), bf16),
            pltpu.VMEM((CHIPS, *block), bf16),
            dma((3,)),
            dma((HEADS,)),
            dma((CHIPS,)),
            dma((HEADS,)),
            dma((CHIPS,)),
            dma((NZ,)),
            dma((NZ,)),
            dma((CHIPS,)),
            dma((HEADS,)),
            pltpu.SemaphoreType.REGULAR((ROWS, NX)),
        ],
        compiler_params=pltpu.CompilerParams(
            collective_id=0, has_side_effects=True, vmem_limit_bytes=54800 * 1024
        ),
    )(queries, keys, values)


def solution(mesh):
    finer = Mesh(mesh.devices.reshape(NZ, NX, 2, mesh.shape["dp"]), ("sp_0", "sp_1", "sp_2", "dp"))
    tokens = P(("dp", "sp_0", "sp_1", "sp_2"), None, None)
    return jax.shard_map(
        shards,
        mesh=finer,
        in_specs=(tokens,) * 3,
        out_specs=P(("dp", "sp_0", "sp_1", "sp_2"), None),
        check_vma=False,
    )
```
